256 devices in a mesh: band: 4 (over x), col: 64 (over z, y, core).
Axes of the slice: x: 4, y: 4, z: 8, core: 2. Of those that a mesh axis runs over, the one named last changes fastest.
Arguments:
- obs_priors: float32 [80, 131072], P(None, ('band', 'col')), may hold values from -0.13258252 to 0.13258252
- innovation: float32 [131072], P(('band', 'col')), may hold values from -6 to 6
- obs_precision: float32 [131072], P(('band', 'col')), may hold values from 0.25 to 4
- tile_block: int32 [1024], P(('band', 'col')), may hold values from 0 to 3
- obs_count: int32 [256], P(('band', 'col')), may hold values from 128 to 512
- block_mask: int32 [4, 256], P(None, 'col'), may hold values 0 or 1
- prior_state_mean: float32 [256, 16, 1024], P('col', None, 'band'), may hold values from -6 to 6
- prior_state_deviation: float32 [256, 16, 80, 1024], P('col', None, None, 'band'), may hold values from -6 to 6
Outputs:
- posterior_mean: float32 [256, 16, 1024], P('col', None, 'band')
- analysis_perturb: float32 [256, 16, 80, 1024], P('col', None, None, 'band')
The draws below stay inside these ranges and needn't reach their ends.
All inputs are finite; a program needn't handle non-finite values. No bound on the sum of `block_mask` on one device may be relied on, other than what follows from the above.
Results may differ from the reference program's by a relative error of at most 0.0001.
Values sent between devices are 32-bit elements; how exact they have to be, the bound alone decides.
No kernel may reach another device: no remote copies, remote signals or barrier semaphores. Data moves between devices by JAX's collectives and lax.ppermute only.
A program may use at most 64 MiB of HBM per device.

```python
import math
import jax
import jax.numpy as jnp
from jax import lax

K = 80
G_DEV = 4
LEV = 16
TILE = 128
TILES_DEV = 4
OBS_DEV = 512
NBANDS = 4
BLOCKS = 256
COLS = 1024
NOBS = 131072
NTILES = 1024
GROUP_COUNT = 256
N_COL = 64


def with_ends(result, key, smallest, top_value):
    place = [jax.random.randint(jax.random.fold_in(key, axis), (), 0, length) for axis, length in enumerate(result.shape)]
    main_axis = result.shape.index(max(result.shape))
    beside = place[:main_axis] + [(place[main_axis] + 1) % result.shape[main_axis]] + place[main_axis + 1:]
    return result.at[tuple(place)].set(smallest).at[tuple(beside)].set(top_value)


def block_levels(own_key, dims, pieces, least, top_value):
    level = 1.0
    for axis_at, shards_of in pieces:
        steps = jax.random.uniform(jax.random.fold_in(jax.random.fold_in(own_key, 6), axis_at), (shards_of,), jnp.float32, least / len(pieces), top_value / len(pieces))
        level = level * jnp.repeat(jnp.exp(steps), dims[axis_at] // shards_of).reshape((-1,) + (1,) * (len(dims) - 1 - axis_at))
    return level


def centred(own_key, extent, scale, reach, pieces=(), held_as=jnp.bfloat16):
    drawn = jax.random.normal(own_key, extent, jnp.float32) * scale
    if len(pieces) > 0:
        drawn = block_levels(own_key, extent, pieces, -0.22, 0.18) * drawn
    return jnp.clip(drawn, min=-reach, max=reach).astype(held_as)


def setup_inputs(seed: int = 0) -> dict:
    keys = jax.random.split(jax.random.key(seed), 9)
    obs_priors = centred(keys[0], (K, NOBS), (4.0 * (N_COL * OBS_DEV) ** -0.5), 0.13258252, ((1, 256),), jnp.float32)
    innovation = centred(keys[1], (NOBS,), 1.0, 6.0, ((0, 256),), jnp.float32)
    obs_precision = jnp.clip(jnp.exp(math.log(4.0) - 2.7725887 * jax.random.uniform(keys[2], (NOBS,), jnp.float32) ** block_levels(keys[2], (NOBS,), ((0, 256),), -0.2, 0.2)), 0.25, 4.0)
    tile_block = with_ends(jax.random.randint(keys[3], (NTILES,), 0, G_DEV), jax.random.fold_in(keys[3], 1), 0, G_DEV - 1).astype(jnp.int32)
    obs_count = with_ends(jax.random.randint(keys[4], (GROUP_COUNT,), TILE, OBS_DEV + 1), jax.random.fold_in(keys[4], 1), TILE, OBS_DEV).astype(jnp.int32)
    block_mask = with_ends((jax.random.randint(keys[5], (NBANDS, BLOCKS), 0, 4) < 3).astype(jnp.int32), jax.random.fold_in(keys[5], 1), 0, 1)
    prior_state_mean = centred(keys[6], (BLOCKS, LEV, COLS), 1.0, 6.0, ((0, 64), (2, 4)), jnp.float32)
    prior_state_deviation = centred(keys[7], (BLOCKS, LEV, K, COLS), 1.0, 6.0, ((0, 64), (3, 4)), jnp.float32)
    return {"obs_priors": obs_priors, "innovation": innovation, "obs_precision": obs_precision, "tile_block": tile_block, "obs_count": obs_count, "block_mask": block_mask, "prior_state_mean": prior_state_mean, "prior_state_deviation": prior_state_deviation}


PRECISION_HIGH = lax.Precision.HIGHEST

def reference(obs_priors, innovation, obs_precision, tile_block, obs_count, block_mask, prior_state_mean, prior_state_deviation):
    ensemble_members = obs_priors.shape[0]
    group_rows = N_COL * OBS_DEV
    identity = jnp.eye(ensemble_members, dtype=jnp.float32)
    affine_update = jnp.concatenate([jnp.broadcast_to(identity, (BLOCKS, ensemble_members, ensemble_members)), jnp.zeros((BLOCKS, ensemble_members, 1), jnp.float32)], axis=2)
    row_index = jnp.arange(OBS_DEV, dtype=jnp.int32)
    col_base = (jnp.arange(N_COL, dtype=jnp.int32) * G_DEV)[:, None]
    for band_index in range(NBANDS):
        priors = obs_priors[:, band_index * group_rows:(band_index + 1) * group_rows].reshape(ensemble_members, N_COL * TILES_DEV, TILE)
        innov_tiles = innovation[band_index * group_rows:(band_index + 1) * group_rows].reshape(N_COL * TILES_DEV, TILE)
        precision_tiles = obs_precision[band_index * group_rows:(band_index + 1) * group_rows]
        counts = obs_count[band_index * N_COL:(band_index + 1) * N_COL]
        live_rows = (row_index[None, :] < counts[:, None]).reshape(N_COL * TILES_DEV, TILE)
        weights = jnp.where(live_rows, precision_tiles.reshape(N_COL * TILES_DEV, TILE), jnp.float32(0.0))
        blocks_here = tile_block[band_index * N_COL * TILES_DEV:(band_index + 1) * N_COL * TILES_DEV].reshape(N_COL, TILES_DEV)
        global_block = (col_base + blocks_here).reshape(-1).astype(jnp.int32)
        tile_maps = affine_update[global_block]
        updated = jnp.einsum('tkl,ktr->ltr', tile_maps, priors, precision=PRECISION_HIGH)
        spread = updated[:ensemble_members]
        departure = innov_tiles - updated[ensemble_members]
        curvature = jnp.einsum('ltr,tr,mtr->lm', spread, weights, spread, precision=PRECISION_HIGH)
        projected = jnp.einsum('ltr,tr->l', spread, weights * departure, precision=PRECISION_HIGH)
        system = (ensemble_members - 1) * identity + curvature
        factor = jnp.linalg.cholesky(system)
        solved = jax.scipy.linalg.cho_solve((factor, True), jnp.concatenate([projected[:, None], curvature], axis=1))
        ensemble_transform = identity - 0.5 * solved[:, 1:]
        augmented = jnp.zeros((ensemble_members + 1, ensemble_members + 1), jnp.float32)
        augmented = augmented.at[:ensemble_members, :ensemble_members].set(ensemble_transform)
        augmented = augmented.at[:ensemble_members, ensemble_members].set(solved[:, 0])
        augmented = augmented.at[ensemble_members, ensemble_members].set(1.0)
        moved = jnp.einsum('gkl,lm->gkm', affine_update, augmented, precision=PRECISION_HIGH)
        apply_flags = block_mask[band_index] > 0
        affine_update = jnp.where(apply_flags[:, None, None], moved, affine_update)
    posterior_mean = prior_state_mean + jnp.einsum('eu,evur->evr', affine_update[:, :, ensemble_members], prior_state_deviation, precision=PRECISION_HIGH)
    analysis_perturb = jnp.einsum('gkm,glkc->glmc', affine_update[:, :, :ensemble_members], prior_state_deviation, precision=PRECISION_HIGH)
    return (posterior_mean, analysis_perturb)
```

```python
import functools

import jax
import jax.numpy as jnp
from jax import lax
from jax.experimental import pallas as pl
from jax.experimental.pallas import tpu as pltpu
from jax.sharding import Mesh
from jax.sharding import PartitionSpec as P

COL = ("col_0", "col_1", "col_2")
BAND_COL = ("band", "col_0", "col_1", "col_2")
HIGHEST = lax.Precision.HIGHEST
LANES = 128
SUB = 8


def lane_of(shape):
    return lax.broadcasted_iota(jnp.int32, shape, 1)


def row_of(shape):
    return lax.broadcasted_iota(jnp.int32, shape, 0)


def matmul(a, b, dims=((1,), (0,))):
    return lax.dot_general(
        a, b, (dims, ((), ())), precision=HIGHEST, preferred_element_type=jnp.float32
    )


def statistics_kernel(
    members,
    band_ref,
    tile_block_ref,
    obs_count_ref,
    block_mask_ref,
    priors_ref,
    innovation_ref,
    precision_ref,
    out_ref,
):
    tiles = tile_block_ref.shape[0]
    tile_rows = priors_ref.shape[1] // tiles
    bands = block_mask_ref.shape[0]
    pairs = 1 << (bands - 2)
    band = band_ref[0]
    count = obs_count_ref[0]
    lane = lane_of((members, LANES))
    row = row_of((members, LANES))
    moments = []
    history = []
    for t in range(tiles):
        cols = pl.ds(t * tile_rows, tile_rows)
        x = priors_ref[:, cols]
        live = (lane_of((1, tile_rows)) + t * tile_rows) < count
        r = jnp.where(live, precision_ref[:, cols], jnp.float32(0.0))
        z = jnp.concatenate(
            [
                x,
                jnp.where(
                    row_of((LANES - members, tile_rows)) == 0, -innovation_ref[:, cols], 0.0
                ),
            ],
            axis=0,
        )
        moments.append(matmul(x * r, z, ((1,), (1,))))
        block = tile_block_ref[t]
        code = jnp.int32(0)
        for j in range(bands - 1):
            applied = jnp.where((block_mask_ref[j, block] > 0) & (j < band), 1 << j, 0)
            code = code + applied
        history.append(code)

    def of_history(s):
        total = jnp.zeros((members, LANES), jnp.float32)
        for t in range(tiles):
            total = total + moments[t] * jnp.where(history[t] == s, 1.0, 0.0)
        return total

    for p in range(pairs):
        even = of_history(2 * p)
        odd = of_history(2 * p + 1)
        packed = jnp.where(lane > row, pltpu.roll(odd, 1, 1), even)
        packed = jnp.where(lane == members + 2, pltpu.roll(even, 2, 1), packed)
        packed = jnp.where(lane > members + 2, 0.0, packed)
        out_ref[pl.ds(p * members, members), :] = packed


def unpack(packed, scratch, members):
    lane = lane_of((members, LANES))
    row = row_of((members, LANES))
    square = jnp.concatenate(
        [packed, jnp.zeros((LANES - members, LANES), jnp.float32)], axis=0
    )
    scratch[...] = square.T
    even = jnp.where(lane <= row, packed, scratch[pl.ds(0, members), :])
    even = jnp.where(lane == members, pltpu.roll(packed, LANES - 2, 1), even)
    even = jnp.where(lane > members, 0.0, even)
    odd = jnp.where(lane >= row, pltpu.roll(packed, LANES - 1, 1), scratch[pl.ds(1, members), :])
    odd = jnp.where(lane > members, 0.0, odd)
    return even, odd


def inverse_and_solution(system, members):
    blocks = members // SUB
    rows = [system[SUB * i : SUB * (i + 1), :] for i in range(blocks)]
    lane = lane_of((SUB, LANES))
    sub = row_of((SUB, LANES))
    for k in range(blocks):
        base = SUB * k
        inside = (lane >= base) & (lane < base + SUB)
        pivot = rows[k]
        spread = [
            jnp.broadcast_to(pivot[:, base + j : base + j + 1], (SUB, LANES)) for j in range(SUB)
        ]
        pivot = jnp.where(inside, jnp.where(lane - base == sub, 1.0, 0.0), pivot)
        for i in range(SUB):
            here = sub == i
            scale = 1.0 / jnp.broadcast_to(spread[i][i : i + 1, :], (SUB, LANES))
            own = jnp.broadcast_to(pivot[i : i + 1, :], (SUB, LANES)) * scale
            factor = spread[i]
            pivot = jnp.where(here, own, pivot - factor * own)
            for j in range(i + 1, SUB):
                other = jnp.broadcast_to(spread[j][i : i + 1, :], (SUB, LANES)) * scale
                spread[j] = jnp.where(here, other, spread[j] - factor * other)
        fresh = [jnp.broadcast_to(pivot[i : i + 1, :], (SUB, LANES)) for i in range(SUB)]
        order = [(k + 1 + m) % blocks for m in range(blocks - 1)]
        for m in order:
            held = rows[m]
            total = jnp.where(inside, 0.0, held)
            for i in range(SUB):
                total = total - held[:, base + i : base + i + 1] * fresh[i]
            rows[m] = total
        rows[k] = pivot
    return jnp.concatenate(rows, axis=0)


def analysis_kernel(
    members,
    block_mask_ref,
    gathered_ref,
    mean_ref,
    deviation_hbm,
    mean_out_ref,
    perturb_hbm,
    deviation,
    perturb,
    maps,
    flip,
    right,
    lhs,
    in_sem,
    out_sem,
):
    bands, groups = block_mask_ref.shape
    levels = mean_ref.shape[1]
    columns = mean_ref.shape[2]
    pairs = 1 << (bands - 2)
    lane = lane_of((members, LANES))
    row = row_of((members, LANES))
    loads = [
        pltpu.make_async_copy(deviation_hbm.at[g], deviation.at[g], in_sem.at[g])
        for g in range(groups)
    ]
    for load in loads:
        load.start()

    by_band = []
    for b in range(bands):
        found = []
        for p in range(max(1, (1 << b) // 2)):
            packed = gathered_ref[pl.ds((b * pairs + p) * members, members), :]
            even, odd = unpack(packed, flip, members)
            found.append(even)
            if b > 0:
                found.append(odd)
        by_band.append(found)

    diagonal = lane == row
    current = [jnp.where(diagonal, 1.0, 0.0) for _ in range(groups)]
    lower = jnp.where(
        (row_of((LANES - members, LANES)) == 0) & (lane_of((LANES - members, LANES)) == members),
        1.0,
        0.0,
    )
    for b in range(bands):
        moment = by_band[b][0]
        system = jnp.where(
            lane == members, -moment, moment + jnp.where(diagonal, members - 1.0, 0.0)
        )
        solved = inverse_and_solution(system, members)
        transform = jnp.where(
            lane < members,
            jnp.where(diagonal, 0.5, 0.0) + (0.5 * (members - 1)) * solved,
            jnp.where(lane == members, solved, 0.0),
        )
        augmented = jnp.concatenate([transform, lower], axis=0)
        for later in range(b + 1, bands):
            held = by_band[later]
            merged = []
            for s in range(0, len(held), 2):
                moved = matmul(held[s + 1], augmented)
                moved = matmul(transform, moved, ((0,), (0,)))[:members, :]
                merged.append(held[s] + moved)
            by_band[later] = merged
        for g in range(groups):
            moved = transform if b == 0 else matmul(current[g], augmented)
            current[g] = jnp.where(block_mask_ref[b, g] > 0, moved, current[g])

    for g in range(groups):
        high = current[g].astype(jnp.bfloat16).astype(jnp.float32)
        low = (current[g] - high).astype(jnp.bfloat16).astype(jnp.float32)
        stack = jnp.concatenate(
            [high, low, high, jnp.zeros((2 * LANES - 3 * members, LANES), jnp.float32)], axis=0
        )
        lhs[g] = stack.T.astype(jnp.bfloat16)

    stores = []
    zero = jnp.zeros((2 * LANES - 3 * members, columns), jnp.bfloat16)
    for g in range(groups):
        loads[g].wait()

        def one_level(l, carry):
            d = deviation[g, l]
            high = d.astype(jnp.bfloat16)
            low = (d - high.astype(jnp.float32)).astype(jnp.bfloat16)
            rhs = jnp.concatenate([high, high, low, zero], axis=0)
            product = jnp.dot(lhs[g], rhs, preferred_element_type=jnp.float32)
            perturb[g, l] = product[:members]
            mean_out_ref[g, pl.ds(l, 1), :] = (
                mean_ref[g, pl.ds(l, 1), :] + product[members : members + 1]
            )
            return carry

        lax.fori_loop(0, levels, one_level, 0, unroll=4)
        store = pltpu.make_async_copy(perturb.at[g], perturb_hbm.at[g], out_sem.at[g])
        store.start()
        stores.append(store)
    for store in stores:
        store.wait()


def local(
    obs_priors,
    innovation,
    obs_precision,
    tile_block,
    obs_count,
    block_mask,
    prior_state_mean,
    prior_state_deviation,
):
    members = obs_priors.shape[0]
    groups, levels, columns = prior_state_mean.shape
    bands = block_mask.shape[0]
    pairs = 1 << (bands - 2)
    parts = lax.axis_size(COL)
    everyone = lax.axis_size(BAND_COL)
    vmem = pl.BlockSpec(memory_space=pltpu.VMEM)
    smem = pl.BlockSpec(memory_space=pltpu.SMEM)
    hbm = pl.BlockSpec(memory_space=pl.ANY)
    my_band = lax.axis_index("band").astype(jnp.int32).reshape(1)
    packed = pl.pallas_call(
        functools.partial(statistics_kernel, members),
        out_shape=jax.ShapeDtypeStruct((pairs * members, LANES), jnp.float32),
        in_specs=[smem] * 4 + [vmem] * 3,
        out_specs=vmem,
    )(
        my_band,
        tile_block,
        obs_count,
        block_mask,
        obs_priors,
        innovation.reshape(1, -1),
        obs_precision.reshape(1, -1),
    )
    share = pairs * members * LANES // parts
    received = lax.all_to_all(packed.reshape(parts, share), COL, 0, 0, tiled=True)
    summed = jnp.sum(received, axis=0, keepdims=True)
    gathered = lax.all_to_all(
        jnp.broadcast_to(summed, (everyone, share)), BAND_COL, 0, 0, tiled=True
    )
    gathered = gathered.reshape(bands * pairs * members, LANES)
    return pl.pallas_call(
        functools.partial(analysis_kernel, members),
        out_shape=(
            jax.ShapeDtypeStruct(prior_state_mean.shape, jnp.float32),
            jax.ShapeDtypeStruct(prior_state_deviation.shape, jnp.float32),
        ),
        in_specs=[smem, vmem, vmem, hbm],
        out_specs=(vmem, hbm),
        scratch_shapes=[
            pltpu.VMEM(prior_state_deviation.shape, jnp.float32),
            pltpu.VMEM(prior_state_deviation.shape, jnp.float32),
            pltpu.VMEM((groups, members, LANES), jnp.float32),
            pltpu.VMEM((LANES, LANES), jnp.float32),
            pltpu.VMEM((LANES, LANES), jnp.float32),
            pltpu.VMEM((groups, LANES, 2 * LANES), jnp.bfloat16),
            pltpu.SemaphoreType.DMA((groups,)),
            pltpu.SemaphoreType.DMA((groups,)),
        ],
    )(block_mask, gathered, prior_state_mean, prior_state_deviation)


def solution(mesh):
    cols = mesh.shape["col"]
    shape = (mesh.shape["band"], cols // 8, 4, 2) if cols % 8 == 0 else (mesh.shape["band"], 1, 1, cols)
    torus = Mesh(mesh.devices.reshape(shape), BAND_COL)
    placed = (
        P(None, BAND_COL),
        P(BAND_COL),
        P(BAND_COL),
        P(BAND_COL),
        P(BAND_COL),
        P(None, COL),
        P(COL, None, "band"),
        P(COL, None, None, "band"),
    )
    return jax.shard_map(
        local,
        mesh=torus,
        in_specs=placed,
        out_specs=(P(COL, None, "band"), P(COL, None, None, "band")),
        check_vma=False,
    )
```

```python
import functools

import jax
import jax.numpy as jnp
from jax import lax
from jax.experimental import pallas as pl
from jax.experimental.pallas import tpu as pltpu
from jax.sharding import Mesh
from jax.sharding import PartitionSpec as P

COL = ("col_0", "col_1", "col_2")
BAND_COL = ("band", "col_0", "col_1", "col_2")
CORE = "col_2"
CORE_FIRST = ("col_2", "col_0", "col_1")
SAME_CORE = ("band", "col_0", "col_1")
HIGHEST = lax.Precision.HIGHEST
LANES = 128
SUB = 8


def lane_of(shape):
    return lax.broadcasted_iota(jnp.int32, shape, 1)


def row_of(shape):
    return lax.broadcasted_iota(jnp.int32, shape, 0)


def matmul(a, b, dims=((1,), (0,))):
    return lax.dot_general(
        a, b, (dims, ((), ())), precision=HIGHEST, preferred_element_type=jnp.float32
    )


def statistics_kernel(
    members,
    band_ref,
    tile_block_ref,
    obs_count_ref,
    block_mask_ref,
    priors_ref,
    innovation_ref,
    precision_ref,
    out_ref,
):
    tiles = tile_block_ref.shape[0]
    tile_rows = priors_ref.shape[1] // tiles
    bands = block_mask_ref.shape[0]
    pairs = 1 << (bands - 2)
    band = band_ref[0]
    count = obs_count_ref[0]
    lane = lane_of((members, LANES))
    row = row_of((members, LANES))
    moments = []
    history = []
    for t in range(tiles):
        cols = pl.ds(t * tile_rows, tile_rows)
        x = priors_ref[:, cols]
        live = (lane_of((1, tile_rows)) + t * tile_rows) < count
        r = jnp.where(live, precision_ref[:, cols], jnp.float32(0.0))
        z = jnp.concatenate(
            [
                x,
                jnp.where(
                    row_of((LANES - members, tile_rows)) == 0, -innovation_ref[:, cols], 0.0
                ),
            ],
            axis=0,
        )
        moments.append(matmul(x * r, z, ((1,), (1,))))
        block = tile_block_ref[t]
        code = jnp.int32(0)
        for j in range(bands - 1):
            applied = jnp.where((block_mask_ref[j, block] > 0) & (j < band), 1 << j, 0)
            code = code + applied
        history.append(code)

    def of_history(s):
        total = jnp.zeros((members, LANES), jnp.float32)
        for t in range(tiles):
            total = total + moments[t] * jnp.where(history[t] == s, 1.0, 0.0)
        return total

    for p in range(pairs):
        even = of_history(2 * p)
        odd = of_history(2 * p + 1)
        packed = jnp.where(lane > row, pltpu.roll(odd, 1, 1), even)
        packed = jnp.where(lane == members + 2, pltpu.roll(even, 2, 1), packed)
        packed = jnp.where(lane > members + 2, 0.0, packed)
        out_ref[pl.ds(p * members, members), :] = packed


def unpack(packed, scratch, members):
    lane = lane_of((members, LANES))
    row = row_of((members, LANES))
    square = jnp.concatenate(
        [packed, jnp.zeros((LANES - members, LANES), jnp.float32)], axis=0
    )
    scratch[...] = square.T
    even = jnp.where(lane <= row, packed, scratch[pl.ds(0, members), :])
    even = jnp.where(lane == members, pltpu.roll(packed, LANES - 2, 1), even)
    even = jnp.where(lane > members, 0.0, even)
    odd = jnp.where(lane >= row, pltpu.roll(packed, LANES - 1, 1), scratch[pl.ds(1, members), :])
    odd = jnp.where(lane > members, 0.0, odd)
    return even, odd


def inverse_and_solution(system, nothing, members):
    blocks = members // SUB
    rows = [system[SUB * i : SUB * (i + 1), :] for i in range(blocks)]
    lane = lane_of((SUB, LANES))
    sub = row_of((SUB, LANES))
    for k in range(blocks):
        base = SUB * k
        inside = (lane >= base) & (lane < base + SUB)
        pivot = rows[k]
        spread = [
            nothing + jnp.broadcast_to(pivot[:, base + j : base + j + 1], (SUB, LANES))
            for j in range(SUB)
        ]
        pivot = jnp.where(inside, jnp.where(lane - base == sub, 1.0, 0.0), pivot)
        for i in range(SUB):
            here = sub == i
            scale = 1.0 / jnp.broadcast_to(spread[i][i : i + 1, :], (SUB, LANES))
            own = jnp.broadcast_to(pivot[i : i + 1, :], (SUB, LANES)) * scale
            factor = spread[i]
            pivot = jnp.where(here, own, pivot - factor * own)
            for j in range(i + 1, SUB):
                other = jnp.broadcast_to(spread[j][i : i + 1, :], (SUB, LANES)) * scale
                spread[j] = jnp.where(here, other, spread[j] - factor * other)
        fresh = [jnp.broadcast_to(pivot[i : i + 1, :], (SUB, LANES)) for i in range(SUB)]
        order = [(k + 1 + m) % blocks for m in range(blocks - 1)]
        for m in order:
            held = rows[m]
            total = jnp.where(inside, 0.0, held)
            for i in range(SUB):
                total = total - held[:, base + i : base + i + 1] * fresh[i]
            rows[m] = total
        rows[k] = pivot
    return jnp.concatenate(rows, axis=0)


def analysis_kernel(
    members,
    block_mask_ref,
    gathered_ref,
    mean_ref,
    deviation_hbm,
    mean_out_ref,
    perturb_hbm,
    deviation,
    perturb,
    nothing,
    flip,
    lhs,
    in_sem,
    out_sem,
):
    bands, groups = block_mask_ref.shape
    levels = mean_ref.shape[1]
    columns = mean_ref.shape[2]
    cores = gathered_ref.shape[0]
    pairs = 1 << (bands - 2)
    lane = lane_of((members, LANES))
    row = row_of((members, LANES))
    loads = [
        pltpu.make_async_copy(deviation_hbm.at[g], deviation.at[g], in_sem.at[g])
        for g in range(groups)
    ]
    for load in loads:
        load.start()
    nothing[...] = jnp.zeros_like(nothing)

    by_band = []
    for b in range(bands):
        found = []
        for p in range(max(1, (1 << b) // 2)):
            half = pairs // cores
            at = (b * half + p % half) * members
            packed = gathered_ref[p // half, pl.ds(at, members), :]
            even, odd = unpack(packed, flip, members)
            found.append(even)
            if b > 0:
                found.append(odd)
        by_band.append(found)

    diagonal = lane == row
    current = [jnp.where(diagonal, 1.0, 0.0) for _ in range(groups)]
    lower = jnp.where(
        (row_of((LANES - members, LANES)) == 0) & (lane_of((LANES - members, LANES)) == members),
        1.0,
        0.0,
    )
    for b in range(bands):
        moment = by_band[b][0]
        system = jnp.where(
            lane == members, -moment, moment + jnp.where(diagonal, members - 1.0, 0.0)
        )
        solved = inverse_and_solution(system, nothing[...], members)
        transform = jnp.where(
            lane < members,
            jnp.where(diagonal, 0.5, 0.0) + (0.5 * (members - 1)) * solved,
            jnp.where(lane == members, solved, 0.0),
        )
        augmented = jnp.concatenate([transform, lower], axis=0)
        for later in range(b + 1, bands):
            held = by_band[later]
            merged = []
            for s in range(0, len(held), 2):
                moved = matmul(held[s + 1], augmented)
                moved = matmul(transform, moved, ((0,), (0,)))[:members, :]
                merged.append(held[s] + moved)
            by_band[later] = merged
        for g in range(groups):
            moved = transform if b == 0 else matmul(current[g], augmented)
            current[g] = jnp.where(block_mask_ref[b, g] > 0, moved, current[g])

    for g in range(groups):
        high = current[g].astype(jnp.bfloat16).astype(jnp.float32)
        low = (current[g] - high).astype(jnp.bfloat16).astype(jnp.float32)
        stack = jnp.concatenate(
            [high, low, high, jnp.zeros((2 * LANES - 3 * members, LANES), jnp.float32)], axis=0
        )
        lhs[g] = stack.T.astype(jnp.bfloat16)

    stores = []
    zero = jnp.zeros((2 * LANES - 3 * members, columns), jnp.bfloat16)
    for g in range(groups):
        loads[g].wait()

        def one_level(l, carry):
            d = deviation[g, l]
            high = d.astype(jnp.bfloat16)
            low = (d - high.astype(jnp.float32)).astype(jnp.bfloat16)
            rhs = jnp.concatenate([high, high, low, zero], axis=0)
            product = jnp.dot(lhs[g], rhs, preferred_element_type=jnp.float32)
            perturb[g, l] = product[:members]
            mean_out_ref[g, pl.ds(l, 1), :] = (
                mean_ref[g, pl.ds(l, 1), :] + product[members : members + 1]
            )
            return carry

        lax.fori_loop(0, levels, one_level, 0, unroll=4)
        store = pltpu.make_async_copy(perturb.at[g], perturb_hbm.at[g], out_sem.at[g])
        store.start()
        stores.append(store)
    for store in stores:
        store.wait()


def local(
    obs_priors,
    innovation,
    obs_precision,
    tile_block,
    obs_count,
    block_mask,
    prior_state_mean,
    prior_state_deviation,
):
    members = obs_priors.shape[0]
    groups, levels, columns = prior_state_mean.shape
    bands = block_mask.shape[0]
    pairs = 1 << (bands - 2)
    parts = lax.axis_size(COL)
    everyone = lax.axis_size(SAME_CORE)
    vmem = pl.BlockSpec(memory_space=pltpu.VMEM)
    smem = pl.BlockSpec(memory_space=pltpu.SMEM)
    hbm = pl.BlockSpec(memory_space=pl.ANY)
    my_band = lax.axis_index("band").astype(jnp.int32).reshape(1)
    packed = pl.pallas_call(
        functools.partial(statistics_kernel, members),
        out_shape=jax.ShapeDtypeStruct((pairs * members, LANES), jnp.float32),
        in_specs=[smem] * 4 + [vmem] * 3,
        out_specs=vmem,
    )(
        my_band,
        tile_block,
        obs_count,
        block_mask,
        obs_priors,
        innovation.reshape(1, -1),
        obs_precision.reshape(1, -1),
    )
    share = pairs * members * LANES // parts
    received = lax.all_to_all(packed.reshape(parts, share), CORE_FIRST, 0, 0, tiled=True)
    summed = jnp.sum(received, axis=0, keepdims=True)
    copies = jnp.broadcast_to(summed, (everyone, share))
    own_half = lax.all_to_all(copies, SAME_CORE, 0, 0, tiled=True)
    own_half = own_half.reshape(-1, LANES)
    gathered = lax.all_gather(own_half, CORE, axis=0, tiled=False)
    return pl.pallas_call(
        functools.partial(analysis_kernel, members),
        out_shape=(
            jax.ShapeDtypeStruct(prior_state_mean.shape, jnp.float32),
            jax.ShapeDtypeStruct(prior_state_deviation.shape, jnp.float32),
        ),
        in_specs=[smem, vmem, vmem, hbm],
        out_specs=(vmem, hbm),
        scratch_shapes=[
            pltpu.VMEM(prior_state_deviation.shape, jnp.float32),
            pltpu.VMEM(prior_state_deviation.shape, jnp.float32),
            pltpu.VMEM((SUB, LANES), jnp.float32),
            pltpu.VMEM((LANES, LANES), jnp.float32),
            pltpu.VMEM((groups, LANES, 2 * LANES), jnp.bfloat16),
            pltpu.SemaphoreType.DMA((groups,)),
            pltpu.SemaphoreType.DMA((groups,)),
        ],
    )(block_mask, gathered, prior_state_mean, prior_state_deviation)


def solution(mesh):
    cols = mesh.shape["col"]
    shape = (mesh.shape["band"], cols // 8, 4, 2) if cols % 8 == 0 else (mesh.shape["band"], 1, 1, cols)
    torus = Mesh(mesh.devices.reshape(shape), BAND_COL)
    placed = (
        P(None, BAND_COL),
        P(BAND_COL),
        P(BAND_COL),
        P(BAND_COL),
        P(BAND_COL),
        P(None, COL),
        P(COL, None, "band"),
        P(COL, None, None, "band"),
    )
    return jax.shard_map(
        local,
        mesh=torus,
        in_specs=placed,
        out_specs=(P(COL, None, "band"), P(COL, None, None, "band")),
        check_vma=False,
    )
```

```python
import functools

import jax
import jax.numpy as jnp
from jax import lax
from jax.experimental import pallas as pl
from jax.experimental.pallas import tpu as pltpu
from jax.sharding import Mesh
from jax.sharding import PartitionSpec as P

COL = ("col_0", "col_1", "col_2")
BAND_COL = ("band", "col_0", "col_1", "col_2")
CORE = "col_2"
CORE_FIRST = ("col_2", "col_0", "col_1")
SAME_CORE = ("band", "col_0", "col_1")
HIGHEST = lax.Precision.HIGHEST
LANES = 128
SUB = 8
START = 83


def lane_of(shape):
    return lax.broadcasted_iota(jnp.int32, shape, 1)


def row_of(shape):
    return lax.broadcasted_iota(jnp.int32, shape, 0)


def matmul(a, b, dims=((1,), (0,))):
    return lax.dot_general(
        a, b, (dims, ((), ())), precision=HIGHEST, preferred_element_type=jnp.float32
    )


def statistics_kernel(
    members,
    band_ref,
    tile_block_ref,
    obs_count_ref,
    block_mask_ref,
    priors_ref,
    innovation_ref,
    precision_ref,
    out_ref,
):
    tiles = tile_block_ref.shape[0]
    tile_rows = priors_ref.shape[1] // tiles
    bands = block_mask_ref.shape[0]
    histories = 1 << (bands - 1)
    band = band_ref[0]
    count = obs_count_ref[0]
    lane = lane_of((members, LANES))
    row = row_of((members, LANES))
    moments = []
    history = []
    for t in range(tiles):
        cols = pl.ds(t * tile_rows, tile_rows)
        x = priors_ref[:, cols]
        live = (lane_of((1, tile_rows)) + t * tile_rows) < count
        r = jnp.where(live, precision_ref[:, cols], jnp.float32(0.0))
        z = jnp.concatenate(
            [
                x,
                jnp.where(
                    row_of((LANES - members, tile_rows)) == 0, -innovation_ref[:, cols], 0.0
                ),
            ],
            axis=0,
        )
        moments.append(matmul(x * r, z, ((1,), (1,))))
        block = tile_block_ref[t]
        code = jnp.int32(0)
        for j in range(bands - 1):
            applied = jnp.where((block_mask_ref[j, block] > 0) & (j < band), 1 << j, 0)
            code = code + applied
        history.append(code)

    def of_history(s):
        total = jnp.zeros((members, LANES), jnp.float32)
        for t in range(tiles):
            total = total + moments[t] * jnp.where(history[t] == s, 1.0, 0.0)
        return total

    half = members // 2
    top = row_of((half, LANES))
    spot = lane_of((half, LANES))
    for q in range(-(-histories // 3)):
        even = of_history(3 * q)
        odd = of_history(3 * q + 1)
        packed = jnp.where(lane > row, pltpu.roll(odd, 1, 1), even)
        packed = jnp.where(lane == members + 2, pltpu.roll(even, 2, 1), packed)
        if 3 * q + 2 < histories:
            third = of_history(3 * q + 2)
            left = pltpu.roll(third, START, 1)
            right = pltpu.roll(third, START + 1 - half, 1)
            upper = jnp.where(spot - START <= top, left[:half], right[half:])
            lower = left[half:]
            below = jnp.concatenate([upper, lower], axis=0)
            below = jnp.where(lane == START + half + 1, right, below)
            below = jnp.where(lane > START + half + 1, 0.0, below)
            packed = jnp.where(lane > members + 2, below, packed)
        else:
            packed = jnp.where(lane > members + 2, 0.0, packed)
        out_ref[pl.ds(q * members, members), :] = packed
    used = -(-histories // 3) * members
    if used < out_ref.shape[0]:
        rest = out_ref.shape[0] - used
        out_ref[pl.ds(used, rest), :] = jnp.zeros((rest, LANES), jnp.float32)


def flipped(value, scratch, members):
    scratch[...] = jnp.concatenate(
        [value, jnp.zeros((LANES - members, LANES), jnp.float32)], axis=0
    ).T


def unpack_two(packed, scratch, members):
    lane = lane_of((members, LANES))
    row = row_of((members, LANES))
    flipped(packed, scratch, members)
    even = jnp.where(lane <= row, packed, scratch[pl.ds(0, members), :])
    even = jnp.where(lane == members, pltpu.roll(packed, LANES - 2, 1), even)
    even = jnp.where(lane > members, 0.0, even)
    odd = jnp.where(lane >= row, pltpu.roll(packed, LANES - 1, 1), scratch[pl.ds(1, members), :])
    odd = jnp.where(lane > members, 0.0, odd)
    return even, odd


def unpack_third(packed, scratch, members):
    half = members // 2
    lane = lane_of((members, LANES))
    row = row_of((members, LANES))
    left = pltpu.roll(packed, LANES - START, 1)
    right = pltpu.roll(packed, LANES - (START + 1 - half), 1)
    corner = jnp.concatenate([right[:half], right[:half]], axis=0)
    once = jnp.where(lane < half, left, corner)
    flipped(jnp.where(lane < members, once, 0.0), scratch, members)
    held = ((lane < half) & ((row >= half) | (lane <= row))) | (
        (lane >= half) & (row >= half) & (lane >= row)
    )
    third = jnp.where(held, once, scratch[pl.ds(0, members), :])
    third = jnp.where(lane == members, right, third)
    return jnp.where(lane > members, 0.0, third)


def inverse_and_solution(system, nothing, members, tasks):
    blocks = members // SUB
    rows = [system[SUB * i : SUB * (i + 1), :] for i in range(blocks)]
    lane = lane_of((SUB, LANES))
    sub = row_of((SUB, LANES))
    issued = 0
    for k in range(blocks):
        base = SUB * k
        inside = (lane >= base) & (lane < base + SUB)
        pivot = rows[k]
        spread = [
            nothing + jnp.broadcast_to(pivot[:, base + j : base + j + 1], (SUB, LANES))
            for j in range(SUB)
        ]
        pivot = jnp.where(inside, jnp.where(lane - base == sub, 1.0, 0.0), pivot)
        for i in range(SUB):
            here = sub == i
            scale = 1.0 / jnp.broadcast_to(spread[i][i : i + 1, :], (SUB, LANES))
            own = jnp.broadcast_to(pivot[i : i + 1, :], (SUB, LANES)) * scale
            factor = spread[i]
            pivot = jnp.where(here, own, pivot - factor * own)
            for j in range(i + 1, SUB):
                other = jnp.broadcast_to(spread[j][i : i + 1, :], (SUB, LANES)) * scale
                spread[j] = jnp.where(here, other, spread[j] - factor * other)
        while issued < len(tasks) * (k + 1) // blocks:
            tasks[issued]()
            issued += 1
        fresh = [jnp.broadcast_to(pivot[i : i + 1, :], (SUB, LANES)) for i in range(SUB)]
        order = [(k + 1 + m) % blocks for m in range(blocks - 1)]
        for m in order:
            held = rows[m]
            total = jnp.where(inside, 0.0, held)
            for i in range(SUB):
                total = total - held[:, base + i : base + i + 1] * fresh[i]
            rows[m] = total
        rows[k] = pivot
    return jnp.concatenate(rows, axis=0)


def analysis_kernel(
    members,
    block_mask_ref,
    core_ref,
    mine_ref,
    other_ref,
    mean_ref,
    deviation_hbm,
    mean_out_ref,
    perturb_hbm,
    deviation,
    perturb,
    nothing,
    flips,
    moments,
    maps,
    transforms,
    lhs,
    in_sem,
    out_sem,
):
    bands, groups = block_mask_ref.shape
    levels = mean_ref.shape[1]
    columns = mean_ref.shape[2]
    lane = lane_of((members, LANES))
    row = row_of((members, LANES))
    diagonal = lane == row
    loads = [
        pltpu.make_async_copy(deviation_hbm.at[g], deviation.at[g], in_sem.at[g])
        for g in range(groups)
    ]
    for load in loads:
        load.start()
    nothing[...] = jnp.zeros_like(nothing)
    lower = jnp.where(
        (row_of((LANES - members, LANES)) == 0) & (lane_of((LANES - members, LANES)) == members),
        1.0,
        0.0,
    )
    for b in range(bands):
        transforms[b, pl.ds(members, LANES - members), :] = lower
    band_rows = mine_ref.shape[0] // bands
    first_core = core_ref[0] == 0

    def tile(b, q):
        pieces = []
        for core in range(2):
            low = max(q * members, core * band_rows)
            high = min((q + 1) * members, (core + 1) * band_rows)
            if low < high:
                at = pl.ds(b * band_rows + low - core * band_rows, high - low)
                mine, other = mine_ref[at, :], other_ref[at, :]
                own = first_core if core == 0 else jnp.logical_not(first_core)
                pieces.append(jnp.where(own, mine, other))
        return pieces[0] if len(pieces) == 1 else jnp.concatenate(pieces, axis=0)

    used = [0]

    def scratch():
        used[0] += 1
        return flips.at[used[0] % flips.shape[0]]

    def slot(b, s):
        return (1 << b) - 1 + s

    def unpack_first(b, q):
        def task():
            even, odd = unpack_two(tile(b, q), scratch(), members)
            moments[slot(b, 3 * q)] = even
            if 3 * q + 1 < (1 << b):
                moments[slot(b, 3 * q + 1)] = odd

        return task

    def unpack_last(b, q):
        def task():
            moments[slot(b, 3 * q + 2)] = unpack_third(tile(b, q), scratch(), members)

        return task

    def merge(stage, b, s):
        def task():
            moved = matmul(moments[slot(b, 2 * s + 1)], transforms[stage])
            square = transforms[stage, pl.ds(0, members), pl.ds(0, members)]
            moments[slot(b, s)] = moments[slot(b, 2 * s)] + matmul(square, moved)

        return task

    def update(stage, g):
        def task():
            new = transforms[stage, pl.ds(0, members), :]
            if stage == 0:
                old = jnp.where(diagonal, 1.0, 0.0)
            else:
                old = maps[g]
                new = matmul(old, transforms[stage])
            maps[g] = jnp.where(block_mask_ref[stage, g] > 0, new, old)

        return task

    unpack_first(0, 0)()
    during = [[] for _ in range(bands)]
    for b in range(1, bands):
        for q in range(-(-(1 << b) // 3)):
            during[0].append(unpack_first(b, q))
            if 3 * q + 2 < (1 << b):
                during[0].append(unpack_last(b, q))
    for stage in range(bands - 1):
        for later in range(stage + 2, bands):
            for s in range(1 << (later - stage - 1)):
                during[stage + 1].append(merge(stage, later, s))
        for g in range(groups):
            during[stage + 1].append(update(stage, g))

    for b in range(bands):
        moment = moments[slot(b, 0)]
        system = jnp.where(
            lane == members, -moment, moment + jnp.where(diagonal, members - 1.0, 0.0)
        )
        solved = inverse_and_solution(system, nothing[...], members, during[b])
        transforms[b, pl.ds(0, members), :] = jnp.where(
            lane < members,
            jnp.where(diagonal, 0.5, 0.0) + (0.5 * (members - 1)) * solved,
            jnp.where(lane == members, solved, 0.0),
        )
        if b + 1 < bands:
            merge(b, b + 1, 0)()

    stores = []
    zero = jnp.zeros((2 * LANES - 3 * members, columns), jnp.bfloat16)
    for g in range(groups):
        update(bands - 1, g)()
        high = maps[g].astype(jnp.bfloat16).astype(jnp.float32)
        low = (maps[g] - high).astype(jnp.bfloat16).astype(jnp.float32)
        stack = jnp.concatenate(
            [high, low, high, jnp.zeros((2 * LANES - 3 * members, LANES), jnp.float32)], axis=0
        )
        lhs[g] = stack.T.astype(jnp.bfloat16)
    for g in range(groups):
        loads[g].wait()

        def one_level(l, carry):
            d = deviation[g, l]
            high = d.astype(jnp.bfloat16)
            low = (d - high.astype(jnp.float32)).astype(jnp.bfloat16)
            rhs = jnp.concatenate([high, high, low, zero], axis=0)
            product = jnp.dot(lhs[g], rhs, preferred_element_type=jnp.float32)
            perturb[g, l] = product[:members]
            mean_out_ref[g, pl.ds(l, 1), :] = (
                mean_ref[g, pl.ds(l, 1), :] + product[members : members + 1]
            )
            return carry

        lax.fori_loop(0, levels, one_level, 0, unroll=4)
        store = pltpu.make_async_copy(perturb.at[g], perturb_hbm.at[g], out_sem.at[g])
        store.start()
        stores.append(store)
    for store in stores:
        store.wait()


def local(
    obs_priors,
    innovation,
    obs_precision,
    tile_block,
    obs_count,
    block_mask,
    prior_state_mean,
    prior_state_deviation,
):
    members = obs_priors.shape[0]
    groups, levels, columns = prior_state_mean.shape
    bands = block_mask.shape[0]
    histories = 1 << (bands - 1)
    parts = lax.axis_size(COL)
    everyone = lax.axis_size(SAME_CORE)
    band_rows = -(-(-(-histories // 3) * members) // parts) * parts
    share = band_rows * LANES // parts
    vmem = pl.BlockSpec(memory_space=pltpu.VMEM)
    smem = pl.BlockSpec(memory_space=pltpu.SMEM)
    hbm = pl.BlockSpec(memory_space=pl.ANY)
    my_band = lax.axis_index("band").astype(jnp.int32).reshape(1)
    packed = pl.pallas_call(
        functools.partial(statistics_kernel, members),
        out_shape=jax.ShapeDtypeStruct((band_rows, LANES), jnp.float32),
        in_specs=[smem] * 4 + [vmem] * 3,
        out_specs=vmem,
        compiler_params=pltpu.CompilerParams(vmem_limit_bytes=8 << 20),
    )(
        my_band,
        tile_block,
        obs_count,
        block_mask,
        obs_priors,
        innovation.reshape(1, -1),
        obs_precision.reshape(1, -1),
    )
    received = lax.all_to_all(packed.reshape(parts, share), CORE_FIRST, 0, 0, tiled=True)
    summed = jnp.sum(received, axis=0, keepdims=True)
    copies = jnp.broadcast_to(summed, (everyone, share))
    mine = lax.all_to_all(copies, SAME_CORE, 0, 0, tiled=True).reshape(-1, LANES)
    other = lax.ppermute(mine, CORE, [(0, 1), (1, 0)])
    my_core = lax.axis_index(CORE).astype(jnp.int32).reshape(1)
    return pl.pallas_call(
        functools.partial(analysis_kernel, members),
        out_shape=(
            jax.ShapeDtypeStruct(prior_state_mean.shape, jnp.float32),
            jax.ShapeDtypeStruct(prior_state_deviation.shape, jnp.float32),
        ),
        in_specs=[smem, smem, vmem, vmem, vmem, hbm],
        out_specs=(vmem, hbm),
        scratch_shapes=[
            pltpu.VMEM(prior_state_deviation.shape, jnp.float32),
            pltpu.VMEM(prior_state_deviation.shape, jnp.float32),
            pltpu.VMEM((SUB, LANES), jnp.float32),
            pltpu.VMEM((4, LANES, LANES), jnp.float32),
            pltpu.VMEM(((1 << bands) - 1, members, LANES), jnp.float32),
            pltpu.VMEM((groups, members, LANES), jnp.float32),
            pltpu.VMEM((bands, LANES, LANES), jnp.float32),
            pltpu.VMEM((groups, LANES, 2 * LANES), jnp.bfloat16),
            pltpu.SemaphoreType.DMA((groups,)),
            pltpu.SemaphoreType.DMA((groups,)),
        ],
        compiler_params=pltpu.CompilerParams(vmem_limit_bytes=50 << 20),
    )(block_mask, my_core, mine, other, prior_state_mean, prior_state_deviation)


def solution(mesh):
    cols = mesh.shape["col"]
    shape = (mesh.shape["band"], cols // 8, 4, 2) if cols % 8 == 0 else (mesh.shape["band"], 1, 1, cols)
    torus = Mesh(mesh.devices.reshape(shape), BAND_COL)
    placed = (
        P(None, BAND_COL),
        P(BAND_COL),
        P(BAND_COL),
        P(BAND_COL),
        P(BAND_COL),
        P(None, COL),
        P(COL, None, "band"),
        P(COL, None, None, "band"),
    )
    return jax.shard_map(
        local,
        mesh=torus,
        in_specs=placed,
        out_specs=(P(COL, None, "band"), P(COL, None, None, "band")),
        check_vma=False,
    )
```

```python
import functools

import jax
import jax.numpy as jnp
from jax import lax
from jax.experimental import pallas as pl
from jax.experimental.pallas import tpu as pltpu
from jax.sharding import Mesh
from jax.sharding import PartitionSpec as P

COL = ("col_0", "col_1", "col_2")
BAND_COL = ("band", "col_0", "col_1", "col_2")
CORE = "col_2"
CORE_FIRST = ("col_2", "col_0", "col_1")
SAME_CORE = ("band", "col_0", "col_1")
HIGHEST = lax.Precision.HIGHEST
LANES = 128
SUB = 8
START = 83


def lane_of(shape):
    return lax.broadcasted_iota(jnp.int32, shape, 1)


def row_of(shape):
    return lax.broadcasted_iota(jnp.int32, shape, 0)


def matmul(a, b, dims=((1,), (0,))):
    return lax.dot_general(
        a, b, (dims, ((), ())), precision=HIGHEST, preferred_element_type=jnp.float32
    )


def statistics_kernel(
    members,
    band_ref,
    tile_block_ref,
    obs_count_ref,
    block_mask_ref,
    priors_ref,
    innovation_ref,
    precision_ref,
    out_ref,
):
    tiles = tile_block_ref.shape[0]
    tile_rows = priors_ref.shape[1] // tiles
    bands = block_mask_ref.shape[0]
    histories = 1 << (bands - 1)
    band = band_ref[0]
    count = obs_count_ref[0]
    lane = lane_of((members, LANES))
    row = row_of((members, LANES))
    moments = []
    history = []
    for t in range(tiles):
        cols = pl.ds(t * tile_rows, tile_rows)
        x = priors_ref[:, cols]
        live = (lane_of((1, tile_rows)) + t * tile_rows) < count
        r = jnp.where(live, precision_ref[:, cols], jnp.float32(0.0))
        z = jnp.concatenate(
            [
                x,
                jnp.where(
                    row_of((LANES - members, tile_rows)) == 0, -innovation_ref[:, cols], 0.0
                ),
            ],
            axis=0,
        )
        moments.append(matmul(x * r, z, ((1,), (1,))))
        block = tile_block_ref[t]
        code = jnp.int32(0)
        for j in range(bands - 1):
            applied = jnp.where((block_mask_ref[j, block] > 0) & (j < band), 1 << j, 0)
            code = code + applied
        history.append(code)

    def of_history(s):
        total = jnp.zeros((members, LANES), jnp.float32)
        for t in range(tiles):
            total = total + moments[t] * jnp.where(history[t] == s, 1.0, 0.0)
        return total

    half = members // 2
    top = row_of((half, LANES))
    spot = lane_of((half, LANES))
    for q in range(-(-histories // 3)):
        even = of_history(3 * q)
        odd = of_history(3 * q + 1)
        packed = jnp.where(lane > row, pltpu.roll(odd, 1, 1), even)
        packed = jnp.where(lane == members + 2, pltpu.roll(even, 2, 1), packed)
        if 3 * q + 2 < histories:
            third = of_history(3 * q + 2)
            left = pltpu.roll(third, START, 1)
            right = pltpu.roll(third, START + 1 - half, 1)
            upper = jnp.where(spot - START <= top, left[:half], right[half:])
            lower = left[half:]
            below = jnp.concatenate([upper, lower], axis=0)
            below = jnp.where(lane == START + half + 1, right, below)
            below = jnp.where(lane > START + half + 1, 0.0, below)
            packed = jnp.where(lane > members + 2, below, packed)
        else:
            packed = jnp.where(lane > members + 2, 0.0, packed)
        out_ref[pl.ds(q * members, members), :] = packed
    used = -(-histories // 3) * members
    if used < out_ref.shape[0]:
        rest = out_ref.shape[0] - used
        out_ref[pl.ds(used, rest), :] = jnp.zeros((rest, LANES), jnp.float32)


def flipped(value, scratch, members):
    scratch[...] = jnp.concatenate(
        [value, jnp.zeros((LANES - members, LANES), jnp.float32)], axis=0
    ).T


def unpack_two(packed, scratch, members):
    lane = lane_of((members, LANES))
    row = row_of((members, LANES))
    flipped(packed, scratch, members)
    even = jnp.where(lane <= row, packed, scratch[pl.ds(0, members), :])
    even = jnp.where(lane == members, pltpu.roll(packed, LANES - 2, 1), even)
    even = jnp.where(lane > members, 0.0, even)
    odd = jnp.where(lane >= row, pltpu.roll(packed, LANES - 1, 1), scratch[pl.ds(1, members), :])
    odd = jnp.where(lane > members, 0.0, odd)
    return even, odd


def unpack_third(packed, scratch, members):
    half = members // 2
    lane = lane_of((members, LANES))
    row = row_of((members, LANES))
    left = pltpu.roll(packed, LANES - START, 1)
    right = pltpu.roll(packed, LANES - (START + 1 - half), 1)
    corner = jnp.concatenate([right[:half], right[:half]], axis=0)
    once = jnp.where(lane < half, left, corner)
    flipped(jnp.where(lane < members, once, 0.0), scratch, members)
    held = ((lane < half) & ((row >= half) | (lane <= row))) | (
        (lane >= half) & (row >= half) & (lane >= row)
    )
    third = jnp.where(held, once, scratch[pl.ds(0, members), :])
    third = jnp.where(lane == members, right, third)
    return jnp.where(lane > members, 0.0, third)


def inverse_and_solution(system, nothing, members, tasks):
    blocks = members // SUB
    rows = [system[SUB * i : SUB * (i + 1), :] for i in range(blocks)]
    lane = lane_of((SUB, LANES))
    sub = row_of((SUB, LANES))
    issued = 0
    for k in range(blocks):
        base = SUB * k
        inside = (lane >= base) & (lane < base + SUB)
        pivot = rows[k]
        spread = [
            nothing + jnp.broadcast_to(pivot[:, base + j : base + j + 1], (SUB, LANES))
            for j in range(SUB)
        ]
        pivot = jnp.where(inside, jnp.where(lane - base == sub, 1.0, 0.0), pivot)
        for i in range(SUB):
            here = sub == i
            scale = 1.0 / jnp.broadcast_to(spread[i][i : i + 1, :], (SUB, LANES))
            own = jnp.broadcast_to(pivot[i : i + 1, :], (SUB, LANES)) * scale
            factor = spread[i]
            pivot = jnp.where(here, own, pivot - factor * own)
            for j in range(i + 1, SUB):
                other = jnp.broadcast_to(spread[j][i : i + 1, :], (SUB, LANES)) * scale
                spread[j] = jnp.where(here, other, spread[j] - factor * other)
        while issued < len(tasks) * (k + 1) // blocks:
            tasks[issued]()
            issued += 1
        fresh = [jnp.broadcast_to(pivot[i : i + 1, :], (SUB, LANES)) for i in range(SUB)]
        order = [(k + 1 + m) % blocks for m in range(blocks - 1)]
        for m in order:
            held = rows[m]
            total = jnp.where(inside, 0.0, held)
            for i in range(SUB):
                total = total - held[:, base + i : base + i + 1] * fresh[i]
            rows[m] = total
        rows[k] = pivot
    return jnp.concatenate(rows, axis=0)


def analysis_kernel(
    members,
    block_mask_ref,
    core_ref,
    mine_ref,
    other_ref,
    mean_ref,
    deviation_hbm,
    mean_out_ref,
    perturb_hbm,
    deviation,
    perturb,
    nothing,
    flips,
    moments,
    maps,
    transforms,
    lhs,
    in_sem,
    out_sem,
):
    bands, groups = block_mask_ref.shape
    levels = mean_ref.shape[1]
    columns = mean_ref.shape[2]
    lane = lane_of((members, LANES))
    row = row_of((members, LANES))
    diagonal = lane == row
    loads = [
        pltpu.make_async_copy(deviation_hbm.at[g], deviation.at[g], in_sem.at[g])
        for g in range(groups)
    ]
    for load in loads:
        load.start()
    nothing[...] = jnp.zeros_like(nothing)
    lower = jnp.where(
        (row_of((LANES - members, LANES)) == 0) & (lane_of((LANES - members, LANES)) == members),
        1.0,
        0.0,
    )
    for b in range(bands):
        transforms[b, pl.ds(members, LANES - members), :] = lower
    band_rows = mine_ref.shape[0] // bands
    first_core = core_ref[0] == 0

    def tile(b, q):
        pieces = []
        for core in range(2):
            low = max(q * members, core * band_rows)
            high = min((q + 1) * members, (core + 1) * band_rows)
            if low < high:
                at = pl.ds(b * band_rows + low - core * band_rows, high - low)
                mine, other = mine_ref[at, :], other_ref[at, :]
                own = first_core if core == 0 else jnp.logical_not(first_core)
                pieces.append(jnp.where(own, mine, other))
        return pieces[0] if len(pieces) == 1 else jnp.concatenate(pieces, axis=0)

    used = [0]

    def scratch():
        used[0] += 1
        return flips.at[used[0] % flips.shape[0]]

    def slot(b, s):
        return (1 << b) - 1 + s

    def unpack_first(b, q):
        def task():
            even, odd = unpack_two(tile(b, q), scratch(), members)
            moments[slot(b, 3 * q)] = even
            if 3 * q + 1 < (1 << b):
                moments[slot(b, 3 * q + 1)] = odd

        return task

    def unpack_last(b, q):
        def task():
            moments[slot(b, 3 * q + 2)] = unpack_third(tile(b, q), scratch(), members)

        return task

    def merge(stage, b, s):
        def task():
            moved = matmul(moments[slot(b, 2 * s + 1)], transforms[stage])
            square = transforms[stage, pl.ds(0, members), pl.ds(0, members)]
            moments[slot(b, s)] = moments[slot(b, 2 * s)] + matmul(square, moved)

        return task

    def update(stage, g):
        def task():
            new = transforms[stage, pl.ds(0, members), :]
            if stage == 0:
                old = jnp.where(diagonal, 1.0, 0.0)
            else:
                old = maps[g]
                new = matmul(old, transforms[stage])
            maps[g] = jnp.where(block_mask_ref[stage, g] > 0, new, old)

        return task

    unpack_first(0, 0)()
    during = [[] for _ in range(bands)]
    for b in range(1, bands):
        for q in range(-(-(1 << b) // 3)):
            during[0].append(unpack_first(b, q))
            if 3 * q + 2 < (1 << b):
                during[0].append(unpack_last(b, q))
    for stage in range(bands - 1):
        for later in range(stage + 2, bands):
            for s in range(1 << (later - stage - 1)):
                during[stage + 1].append(merge(stage, later, s))
        for g in range(groups):
            during[stage + 1].append(update(stage, g))

    for b in range(bands):
        moment = moments[slot(b, 0)]
        system = jnp.where(
            lane == members, -moment, moment + jnp.where(diagonal, members - 1.0, 0.0)
        )
        solved = inverse_and_solution(system, nothing[...], members, during[b])
        transforms[b, pl.ds(0, members), :] = jnp.where(
            lane < members,
            jnp.where(diagonal, 0.5, 0.0) + (0.5 * (members - 1)) * solved,
            jnp.where(lane == members, solved, 0.0),
        )
        if b + 1 < bands:
            merge(b, b + 1, 0)()

    stores = []
    zero = jnp.zeros((2 * LANES - 3 * members, columns), jnp.bfloat16)
    for g in range(groups):
        update(bands - 1, g)()
        high = maps[g].astype(jnp.bfloat16).astype(jnp.float32)
        low = (maps[g] - high).astype(jnp.bfloat16).astype(jnp.float32)
        stack = jnp.concatenate(
            [high, low, high, jnp.zeros((2 * LANES - 3 * members, LANES), jnp.float32)], axis=0
        )
        lhs[g] = stack.T.astype(jnp.bfloat16)
    for g in range(groups):
        loads[g].wait()

        def one_level(l, carry):
            d = deviation[g, l]
            high = d.astype(jnp.bfloat16)
            low = (d - high.astype(jnp.float32)).astype(jnp.bfloat16)
            rhs = jnp.concatenate([high, high, low, zero], axis=0)
            product = jnp.dot(lhs[g], rhs, preferred_element_type=jnp.float32)
            perturb[g, l] = product[:members]
            mean_out_ref[g, pl.ds(l, 1), :] = (
                mean_ref[g, pl.ds(l, 1), :] + product[members : members + 1]
            )
            return carry

        lax.fori_loop(0, levels, one_level, 0, unroll=4)
        store = pltpu.make_async_copy(perturb.at[g], perturb_hbm.at[g], out_sem.at[g])
        store.start()
        stores.append(store)
    for store in stores:
        store.wait()


def local(
    obs_priors,
    innovation,
    obs_precision,
    tile_block,
    obs_count,
    block_mask,
    prior_state_mean,
    prior_state_deviation,
):
    members = obs_priors.shape[0]
    in_hbm = functools.partial(pltpu.with_memory_space_constraint, memory_space=pltpu.HBM)
    groups, levels, columns = prior_state_mean.shape
    bands = block_mask.shape[0]
    histories = 1 << (bands - 1)
    parts = lax.axis_size(COL)
    everyone = lax.axis_size(SAME_CORE)
    band_rows = -(-(-(-histories // 3) * members) // parts) * parts
    share = band_rows * LANES // parts
    vmem = pl.BlockSpec(memory_space=pltpu.VMEM)
    smem = pl.BlockSpec(memory_space=pltpu.SMEM)
    hbm = pl.BlockSpec(memory_space=pl.ANY)
    my_band = lax.axis_index("band").astype(jnp.int32).reshape(1)
    packed = pl.pallas_call(
        functools.partial(statistics_kernel, members),
        out_shape=jax.ShapeDtypeStruct((band_rows, LANES), jnp.float32),
        in_specs=[smem] * 4 + [vmem] * 3,
        out_specs=vmem,
        compiler_params=pltpu.CompilerParams(vmem_limit_bytes=8 << 20),
    )(
        my_band,
        in_hbm(tile_block),
        obs_count,
        in_hbm(block_mask),
        in_hbm(obs_priors),
        in_hbm(innovation.reshape(1, -1)),
        in_hbm(obs_precision.reshape(1, -1)),
    )
    received = lax.all_to_all(packed.reshape(parts, share), CORE_FIRST, 0, 0, tiled=True)
    summed = jnp.sum(received, axis=0, keepdims=True)
    copies = jnp.broadcast_to(summed, (everyone, share))
    mine = lax.all_to_all(copies, SAME_CORE, 0, 0, tiled=True).reshape(-1, LANES)
    other = lax.ppermute(mine, CORE, [(0, 1), (1, 0)])
    my_core = lax.axis_index(CORE).astype(jnp.int32).reshape(1)
    return pl.pallas_call(
        functools.partial(analysis_kernel, members),
        out_shape=(
            jax.ShapeDtypeStruct(prior_state_mean.shape, jnp.float32),
            jax.ShapeDtypeStruct(prior_state_deviation.shape, jnp.float32),
        ),
        in_specs=[smem, smem, vmem, vmem, vmem, hbm],
        out_specs=(vmem, hbm),
        scratch_shapes=[
            pltpu.VMEM(prior_state_deviation.shape, jnp.float32),
            pltpu.VMEM(prior_state_deviation.shape, jnp.float32),
            pltpu.VMEM((SUB, LANES), jnp.float32),
            pltpu.VMEM((4, LANES, LANES), jnp.float32),
            pltpu.VMEM(((1 << bands) - 1, members, LANES), jnp.float32),
            pltpu.VMEM((groups, members, LANES), jnp.float32),
            pltpu.VMEM((bands, LANES, LANES), jnp.float32),
            pltpu.VMEM((groups, LANES, 2 * LANES), jnp.bfloat16),
            pltpu.SemaphoreType.DMA((groups,)),
            pltpu.SemaphoreType.DMA((groups,)),
        ],
        compiler_params=pltpu.CompilerParams(vmem_limit_bytes=50 << 20),
    )(in_hbm(block_mask), my_core, mine, other, in_hbm(prior_state_mean), in_hbm(prior_state_deviation))


def solution(mesh):
    cols = mesh.shape["col"]
    shape = (mesh.shape["band"], cols // 8, 4, 2) if cols % 8 == 0 else (mesh.shape["band"], 1, 1, cols)
    torus = Mesh(mesh.devices.reshape(shape), BAND_COL)
    placed = (
        P(None, BAND_COL),
        P(BAND_COL),
        P(BAND_COL),
        P(BAND_COL),
        P(BAND_COL),
        P(None, COL),
        P(COL, None, "band"),
        P(COL, None, None, "band"),
    )
    return jax.shard_map(
        local,
        mesh=torus,
        in_specs=placed,
        out_specs=(P(COL, None, "band"), P(COL, None, None, "band")),
        check_vma=False,
    )
```

```python
import functools

import jax
import jax.numpy as jnp
from jax import lax
from jax.experimental import pallas as pl
from jax.experimental.pallas import tpu as pltpu
from jax.sharding import Mesh
from jax.sharding import PartitionSpec as P

COL = ("col_0", "col_1", "col_2")
BAND_COL = ("band", "col_0", "col_1", "col_2")
CORE = "col_2"
CORE_FIRST = ("col_2", "col_0", "col_1")
SAME_CORE = ("band", "col_0", "col_1")
HIGHEST = lax.Precision.HIGHEST
LANES = 128
SUB = 8
START = 83


def lane_of(shape):
    return lax.broadcasted_iota(jnp.int32, shape, 1)


def row_of(shape):
    return lax.broadcasted_iota(jnp.int32, shape, 0)


def matmul(a, b, dims=((1,), (0,))):
    return lax.dot_general(
        a, b, (dims, ((), ())), precision=HIGHEST, preferred_element_type=jnp.float32
    )


def statistics_kernel(
    members,
    band_ref,
    tile_block_ref,
    obs_count_ref,
    block_mask_ref,
    priors_ref,
    innovation_ref,
    precision_ref,
    out_ref,
):
    tiles = tile_block_ref.shape[0]
    tile_rows = priors_ref.shape[1] // tiles
    bands = block_mask_ref.shape[0]
    histories = 1 << (bands - 1)
    band = band_ref[0]
    count = obs_count_ref[0]
    lane = lane_of((members, LANES))
    row = row_of((members, LANES))
    moments = []
    history = []
    for t in range(tiles):
        cols = pl.ds(t * tile_rows, tile_rows)
        x = priors_ref[:, cols]
        live = (lane_of((1, tile_rows)) + t * tile_rows) < count
        r = jnp.where(live, precision_ref[:, cols], jnp.float32(0.0))
        z = jnp.concatenate(
            [
                x,
                jnp.where(
                    row_of((LANES - members, tile_rows)) == 0, -innovation_ref[:, cols], 0.0
                ),
            ],
            axis=0,
        )
        moments.append(matmul(x * r, z, ((1,), (1,))))
        block = tile_block_ref[t]
        code = jnp.int32(0)
        for j in range(bands - 1):
            applied = jnp.where((block_mask_ref[j, block] > 0) & (j < band), 1 << j, 0)
            code = code + applied
        history.append(code)

    def of_history(s):
        total = jnp.zeros((members, LANES), jnp.float32)
        for t in range(tiles):
            total = total + moments[t] * jnp.where(history[t] == s, 1.0, 0.0)
        return total

    half = members // 2
    top = row_of((half, LANES))
    spot = lane_of((half, LANES))
    for q in range(-(-histories // 3)):
        even = of_history(3 * q)
        odd = of_history(3 * q + 1)
        packed = jnp.where(lane > row, pltpu.roll(odd, 1, 1), even)
        packed = jnp.where(lane == members + 2, pltpu.roll(even, 2, 1), packed)
        if 3 * q + 2 < histories:
            third = of_history(3 * q + 2)
            left = pltpu.roll(third, START, 1)
            right = pltpu.roll(third, START + 1 - half, 1)
            upper = jnp.where(spot - START <= top, left[:half], right[half:])
            lower = left[half:]
            below = jnp.concatenate([upper, lower], axis=0)
            below = jnp.where(lane == START + half + 1, right, below)
            below = jnp.where(lane > START + half + 1, 0.0, below)
            packed = jnp.where(lane > members + 2, below, packed)
        else:
            packed = jnp.where(lane > members + 2, 0.0, packed)
        out_ref[pl.ds(q * members, members), :] = packed
    used = -(-histories // 3) * members
    if used < out_ref.shape[0]:
        rest = out_ref.shape[0] - used
        out_ref[pl.ds(used, rest), :] = jnp.zeros((rest, LANES), jnp.float32)


def flipped(value, scratch, members):
    scratch[...] = jnp.concatenate(
        [value, jnp.zeros((LANES - members, LANES), jnp.float32)], axis=0
    ).T


def unpack_two(packed, scratch, members):
    lane = lane_of((members, LANES))
    row = row_of((members, LANES))
    flipped(packed, scratch, members)
    even = jnp.where(lane <= row, packed, scratch[pl.ds(0, members), :])
    even = jnp.where(lane == members, pltpu.roll(packed, LANES - 2, 1), even)
    even = jnp.where(lane > members, 0.0, even)
    odd = jnp.where(lane >= row, pltpu.roll(packed, LANES - 1, 1), scratch[pl.ds(1, members), :])
    odd = jnp.where(lane > members, 0.0, odd)
    return even, odd


def unpack_third(packed, scratch, members):
    half = members // 2
    lane = lane_of((members, LANES))
    row = row_of((members, LANES))
    left = pltpu.roll(packed, LANES - START, 1)
    right = pltpu.roll(packed, LANES - (START + 1 - half), 1)
    corner = jnp.concatenate([right[:half], right[:half]], axis=0)
    once = jnp.where(lane < half, left, corner)
    flipped(jnp.where(lane < members, once, 0.0), scratch, members)
    held = ((lane < half) & ((row >= half) | (lane <= row))) | (
        (lane >= half) & (row >= half) & (lane >= row)
    )
    third = jnp.where(held, once, scratch[pl.ds(0, members), :])
    third = jnp.where(lane == members, right, third)
    return jnp.where(lane > members, 0.0, third)


def row_at(value, i):
    return jnp.broadcast_to(value[i : i + 1, :], (SUB, LANES))


def inverse_and_solution(system, nothing, members, tasks):
    blocks = members // SUB
    rows = [system[SUB * i : SUB * (i + 1), :] for i in range(blocks)]
    lane = lane_of((SUB, LANES))
    sub = row_of((SUB, LANES))
    issued = 0
    for k in range(blocks):
        base = SUB * k
        inside = (lane >= base) & (lane < base + SUB)
        pivot = rows[k]
        spread = [
            nothing + jnp.broadcast_to(pivot[:, base + j : base + j + 1], (SUB, LANES))
            for j in range(SUB)
        ]
        pivot = jnp.where(inside, jnp.where(lane - base == sub, 1.0, 0.0), pivot)
        for i in range(0, SUB, 2):
            first, second = sub == i, sub == i + 1
            one, two = spread[i], spread[i + 1]
            a, b = row_at(one, i), row_at(two, i)
            c, d = row_at(one, i + 1), row_at(two, i + 1)
            scale = 1.0 / (a * d - b * c)

            def eliminated(value):
                top, low = row_at(value, i), row_at(value, i + 1)
                own = (d * top - b * low) * scale
                next_own = (a * low - c * top) * scale
                rest = value - one * own - two * next_own
                return jnp.where(first, own, jnp.where(second, next_own, rest))

            for j in range(i + 2, SUB):
                spread[j] = eliminated(spread[j])
            pivot = eliminated(pivot)
        while issued < len(tasks) * (k + 1) // blocks:
            tasks[issued]()
            issued += 1
        fresh = [row_at(pivot, i) for i in range(SUB)]
        order = [(k + 1 + m) % blocks for m in range(blocks - 1)]
        for m in order:
            held = rows[m]
            total = jnp.where(inside, 0.0, held)
            for i in range(SUB):
                total = total - held[:, base + i : base + i + 1] * fresh[i]
            rows[m] = total
        rows[k] = pivot
    return jnp.concatenate(rows, axis=0)


def analysis_kernel(
    members,
    block_mask_ref,
    core_ref,
    mine_ref,
    other_ref,
    mean_ref,
    deviation_hbm,
    mean_out_ref,
    perturb_hbm,
    deviation,
    perturb,
    nothing,
    flips,
    moments,
    maps,
    transforms,
    lhs,
    in_sem,
    out_sem,
):
    bands, groups = block_mask_ref.shape
    levels = mean_ref.shape[1]
    columns = mean_ref.shape[2]
    lane = lane_of((members, LANES))
    row = row_of((members, LANES))
    diagonal = lane == row
    loads = [
        pltpu.make_async_copy(deviation_hbm.at[g], deviation.at[g], in_sem.at[g])
        for g in range(groups)
    ]
    for load in loads:
        load.start()
    nothing[...] = jnp.zeros_like(nothing)
    lower = jnp.where(
        (row_of((LANES - members, LANES)) == 0) & (lane_of((LANES - members, LANES)) == members),
        1.0,
        0.0,
    )
    for b in range(bands):
        transforms[b, pl.ds(members, LANES - members), :] = lower
    band_rows = mine_ref.shape[0] // bands
    first_core = core_ref[0] == 0

    def tile(b, q):
        pieces = []
        for core in range(2):
            low = max(q * members, core * band_rows)
            high = min((q + 1) * members, (core + 1) * band_rows)
            if low < high:
                at = pl.ds(b * band_rows + low - core * band_rows, high - low)
                mine, other = mine_ref[at, :], other_ref[at, :]
                own = first_core if core == 0 else jnp.logical_not(first_core)
                pieces.append(jnp.where(own, mine, other))
        return pieces[0] if len(pieces) == 1 else jnp.concatenate(pieces, axis=0)

    used = [0]

    def scratch():
        used[0] += 1
        return flips.at[used[0] % flips.shape[0]]

    def slot(b, s):
        return (1 << b) - 1 + s

    def unpack_first(b, q):
        def task():
            even, odd = unpack_two(tile(b, q), scratch(), members)
            moments[slot(b, 3 * q)] = even
            if 3 * q + 1 < (1 << b):
                moments[slot(b, 3 * q + 1)] = odd

        return task

    def unpack_last(b, q):
        def task():
            moments[slot(b, 3 * q + 2)] = unpack_third(tile(b, q), scratch(), members)

        return task

    def merge(stage, b, s):
        def task():
            moved = matmul(moments[slot(b, 2 * s + 1)], transforms[stage])
            square = transforms[stage, pl.ds(0, members), pl.ds(0, members)]
            moments[slot(b, s)] = moments[slot(b, 2 * s)] + matmul(square, moved)

        return task

    def update(stage):
        def task():
            if stage > 0:
                moved = matmul(maps[...], transforms[stage])
            for g in range(groups):
                at = pl.ds(g * members, members)
                if stage == 0:
                    old = jnp.where(diagonal, 1.0, 0.0)
                    new = transforms[stage, pl.ds(0, members), :]
                else:
                    old = maps[at, :]
                    new = moved[g * members : (g + 1) * members, :]
                maps[at, :] = jnp.where(block_mask_ref[stage, g] > 0, new, old)

        return task

    unpack_first(0, 0)()
    during = [[] for _ in range(bands)]
    for b in range(1, bands):
        for q in range(-(-(1 << b) // 3)):
            during[0].append(unpack_first(b, q))
            if 3 * q + 2 < (1 << b):
                during[0].append(unpack_last(b, q))
    for stage in range(bands - 1):
        for later in range(stage + 2, bands):
            for s in range(1 << (later - stage - 1)):
                during[stage + 1].append(merge(stage, later, s))
        during[stage + 1].append(update(stage))

    for b in range(bands):
        moment = moments[slot(b, 0)]
        system = jnp.where(
            lane == members, -moment, moment + jnp.where(diagonal, members - 1.0, 0.0)
        )
        solved = inverse_and_solution(system, nothing[...], members, during[b])
        transforms[b, pl.ds(0, members), :] = jnp.where(
            lane < members,
            jnp.where(diagonal, 0.5, 0.0) + (0.5 * (members - 1)) * solved,
            jnp.where(lane == members, solved, 0.0),
        )
        if b + 1 < bands:
            merge(b, b + 1, 0)()

    stores = []
    zero = jnp.zeros((2 * LANES - 3 * members, columns), jnp.bfloat16)
    update(bands - 1)()
    for g in range(groups):
        final = maps[pl.ds(g * members, members), :]
        high = final.astype(jnp.bfloat16).astype(jnp.float32)
        low = (final - high).astype(jnp.bfloat16).astype(jnp.float32)
        stack = jnp.concatenate(
            [high, low, high, jnp.zeros((2 * LANES - 3 * members, LANES), jnp.float32)], axis=0
        )
        lhs[g] = stack.T.astype(jnp.bfloat16)
    for g in range(groups):
        loads[g].wait()

        def one_level(l, carry):
            d = deviation[g, l]
            high = d.astype(jnp.bfloat16)
            low = (d - high.astype(jnp.float32)).astype(jnp.bfloat16)
            rhs = jnp.concatenate([high, high, low, zero], axis=0)
            product = jnp.dot(lhs[g], rhs, preferred_element_type=jnp.float32)
            perturb[g, l] = product[:members]
            mean_out_ref[g, pl.ds(l, 1), :] = (
                mean_ref[g, pl.ds(l, 1), :] + product[members : members + 1]
            )
            return carry

        lax.fori_loop(0, levels, one_level, 0, unroll=4)
        store = pltpu.make_async_copy(perturb.at[g], perturb_hbm.at[g], out_sem.at[g])
        store.start()
        stores.append(store)
    for store in stores:
        store.wait()


def local(
    obs_priors,
    innovation,
    obs_precision,
    tile_block,
    obs_count,
    block_mask,
    prior_state_mean,
    prior_state_deviation,
):
    members = obs_priors.shape[0]
    in_hbm = functools.partial(pltpu.with_memory_space_constraint, memory_space=pltpu.HBM)
    groups, levels, columns = prior_state_mean.shape
    bands = block_mask.shape[0]
    histories = 1 << (bands - 1)
    parts = lax.axis_size(COL)
    everyone = lax.axis_size(SAME_CORE)
    band_rows = -(-(-(-histories // 3) * members) // parts) * parts
    share = band_rows * LANES // parts
    vmem = pl.BlockSpec(memory_space=pltpu.VMEM)
    smem = pl.BlockSpec(memory_space=pltpu.SMEM)
    hbm = pl.BlockSpec(memory_space=pl.ANY)
    my_band = lax.axis_index("band").astype(jnp.int32).reshape(1)
    packed = pl.pallas_call(
        functools.partial(statistics_kernel, members),
        out_shape=jax.ShapeDtypeStruct((band_rows, LANES), jnp.float32),
        in_specs=[smem] * 4 + [vmem] * 3,
        out_specs=vmem,
        compiler_params=pltpu.CompilerParams(vmem_limit_bytes=8 << 20),
    )(
        my_band,
        in_hbm(tile_block),
        obs_count,
        in_hbm(block_mask),
        in_hbm(obs_priors),
        in_hbm(innovation.reshape(1, -1)),
        in_hbm(obs_precision.reshape(1, -1)),
    )
    received = lax.all_to_all(packed.reshape(parts, share), CORE_FIRST, 0, 0, tiled=True)
    summed = jnp.sum(received, axis=0, keepdims=True)
    copies = jnp.broadcast_to(summed, (everyone, share))
    mine = lax.all_to_all(copies, SAME_CORE, 0, 0, tiled=True).reshape(-1, LANES)
    other = lax.ppermute(mine, CORE, [(0, 1), (1, 0)])
    my_core = lax.axis_index(CORE).astype(jnp.int32).reshape(1)
    return pl.pallas_call(
        functools.partial(analysis_kernel, members),
        out_shape=(
            jax.ShapeDtypeStruct(prior_state_mean.shape, jnp.float32),
            jax.ShapeDtypeStruct(prior_state_deviation.shape, jnp.float32),
        ),
        in_specs=[smem, smem, vmem, vmem, vmem, hbm],
        out_specs=(vmem, hbm),
        scratch_shapes=[
            pltpu.VMEM(prior_state_deviation.shape, jnp.float32),
            pltpu.VMEM(prior_state_deviation.shape, jnp.float32),
            pltpu.VMEM((SUB, LANES), jnp.float32),
            pltpu.VMEM((4, LANES, LANES), jnp.float32),
            pltpu.VMEM(((1 << bands) - 1, members, LANES), jnp.float32),
            pltpu.VMEM((groups * members, LANES), jnp.float32),
            pltpu.VMEM((bands, LANES, LANES), jnp.float32),
            pltpu.VMEM((groups, LANES, 2 * LANES), jnp.bfloat16),
            pltpu.SemaphoreType.DMA((groups,)),
            pltpu.SemaphoreType.DMA((groups,)),
        ],
        compiler_params=pltpu.CompilerParams(vmem_limit_bytes=50 << 20),
    )(in_hbm(block_mask), my_core, mine, other, in_hbm(prior_state_mean), in_hbm(prior_state_deviation))


def solution(mesh):
    cols = mesh.shape["col"]
    shape = (mesh.shape["band"], cols // 8, 4, 2) if cols % 8 == 0 else (mesh.shape["band"], 1, 1, cols)
    torus = Mesh(mesh.devices.reshape(shape), BAND_COL)
    placed = (
        P(None, BAND_COL),
        P(BAND_COL),
        P(BAND_COL),
        P(BAND_COL),
        P(BAND_COL),
        P(None, COL),
        P(COL, None, "band"),
        P(COL, None, None, "band"),
    )
    return jax.shard_map(
        local,
        mesh=torus,
        in_specs=placed,
        out_specs=(P(COL, None, "band"), P(COL, None, None, "band")),
        check_vma=False,
    )
```

```python
import functools

import jax
import jax.numpy as jnp
from jax import lax
from jax.experimental import pallas as pl
from jax.experimental.pallas import tpu as pltpu
from jax.sharding import Mesh
from jax.sharding import PartitionSpec as P

COL = ("col_0", "col_1", "col_2")
BAND_COL = ("band", "col_0", "col_1", "col_2")
CORE = "col_2"
CORE_FIRST = ("col_2", "col_0", "col_1")
SAME_CORE = ("band", "col_0", "col_1")
HIGHEST = lax.Precision.HIGHEST
LANES = 128
SUB = 8
START = 83


def lane_of(shape):
    return lax.broadcasted_iota(jnp.int32, shape, 1)


def row_of(shape):
    return lax.broadcasted_iota(jnp.int32, shape, 0)


def matmul(a, b, dims=((1,), (0,))):
    return lax.dot_general(
        a, b, (dims, ((), ())), precision=HIGHEST, preferred_element_type=jnp.float32
    )


def statistics_kernel(
    members,
    band_ref,
    tile_block_ref,
    obs_count_ref,
    block_mask_ref,
    priors_ref,
    innovation_ref,
    precision_ref,
    out_ref,
):
    tiles = tile_block_ref.shape[0]
    tile_rows = priors_ref.shape[1] // tiles
    bands = block_mask_ref.shape[0]
    histories = 1 << (bands - 1)
    band = band_ref[0]
    count = obs_count_ref[0]
    lane = lane_of((members, LANES))
    row = row_of((members, LANES))
    moments = []
    history = []
    for t in range(tiles):
        cols = pl.ds(t * tile_rows, tile_rows)
        x = priors_ref[:, cols]
        live = (lane_of((1, tile_rows)) + t * tile_rows) < count
        r = jnp.where(live, precision_ref[:, cols], jnp.float32(0.0))
        z = jnp.concatenate(
            [
                x,
                jnp.where(
                    row_of((LANES - members, tile_rows)) == 0, -innovation_ref[:, cols], 0.0
                ),
            ],
            axis=0,
        )
        moments.append(matmul(x * r, z, ((1,), (1,))))
        block = tile_block_ref[t]
        code = jnp.int32(0)
        for j in range(bands - 1):
            applied = jnp.where((block_mask_ref[j, block] > 0) & (j < band), 1 << j, 0)
            code = code + applied
        history.append(code)

    def of_history(s):
        total = jnp.zeros((members, LANES), jnp.float32)
        for t in range(tiles):
            total = total + moments[t] * jnp.where(history[t] == s, 1.0, 0.0)
        return total

    half = members // 2
    top = row_of((half, LANES))
    spot = lane_of((half, LANES))
    for q in range(-(-histories // 3)):
        even = of_history(3 * q)
        odd = of_history(3 * q + 1)
        packed = jnp.where(lane > row, pltpu.roll(odd, 1, 1), even)
        packed = jnp.where(lane == members + 2, pltpu.roll(even, 2, 1), packed)
        if 3 * q + 2 < histories:
            third = of_history(3 * q + 2)
            left = pltpu.roll(third, START, 1)
            right = pltpu.roll(third, START + 1 - half, 1)
            upper = jnp.where(spot - START <= top, left[:half], right[half:])
            lower = left[half:]
            below = jnp.concatenate([upper, lower], axis=0)
            below = jnp.where(lane == START + half + 1, right, below)
            below = jnp.where(lane > START + half + 1, 0.0, below)
            packed = jnp.where(lane > members + 2, below, packed)
        else:
            packed = jnp.where(lane > members + 2, 0.0, packed)
        out_ref[pl.ds(q * members, members), :] = packed
    used = -(-histories // 3) * members
    if used < out_ref.shape[0]:
        rest = out_ref.shape[0] - used
        out_ref[pl.ds(used, rest), :] = jnp.zeros((rest, LANES), jnp.float32)


def flipped(value, scratch, members):
    scratch[...] = jnp.concatenate(
        [value, jnp.zeros((LANES - members, LANES), jnp.float32)], axis=0
    ).T


def unpack_two(packed, scratch, members):
    lane = lane_of((members, LANES))
    row = row_of((members, LANES))
    flipped(packed, scratch, members)
    even = jnp.where(lane <= row, packed, scratch[pl.ds(0, members), :])
    even = jnp.where(lane == members, pltpu.roll(packed, LANES - 2, 1), even)
    even = jnp.where(lane > members, 0.0, even)
    odd = jnp.where(lane >= row, pltpu.roll(packed, LANES - 1, 1), scratch[pl.ds(1, members), :])
    odd = jnp.where(lane > members, 0.0, odd)
    return even, odd


def unpack_third(packed, scratch, members):
    half = members // 2
    lane = lane_of((members, LANES))
    row = row_of((members, LANES))
    left = pltpu.roll(packed, LANES - START, 1)
    right = pltpu.roll(packed, LANES - (START + 1 - half), 1)
    corner = jnp.concatenate([right[:half], right[:half]], axis=0)
    once = jnp.where(lane < half, left, corner)
    flipped(jnp.where(lane < members, once, 0.0), scratch, members)
    held = ((lane < half) & ((row >= half) | (lane <= row))) | (
        (lane >= half) & (row >= half) & (lane >= row)
    )
    third = jnp.where(held, once, scratch[pl.ds(0, members), :])
    third = jnp.where(lane == members, right, third)
    return jnp.where(lane > members, 0.0, third)


def row_at(value, i):
    return jnp.broadcast_to(value[i : i + 1, :], (SUB, LANES))


def inverse_and_solution(system, nothing, members, tasks):
    blocks = members // SUB
    rows = [system[SUB * i : SUB * (i + 1), :] for i in range(blocks)]
    lane = lane_of((SUB, LANES))
    sub = row_of((SUB, LANES))
    issued = 0
    for k in range(blocks):
        base = SUB * k
        inside = (lane >= base) & (lane < base + SUB)
        pivot = rows[k]
        spread = [
            nothing + jnp.broadcast_to(pivot[:, base + j : base + j + 1], (SUB, LANES))
            for j in range(SUB)
        ]
        pivot = jnp.where(inside, jnp.where(lane - base == sub, 1.0, 0.0), pivot)
        for i in range(0, SUB, 2):
            first, second = sub == i, sub == i + 1
            one, two = spread[i], spread[i + 1]
            a, b = row_at(one, i), row_at(two, i)
            c, d = row_at(one, i + 1), row_at(two, i + 1)
            scale = 1.0 / (a * d - b * c)
            a, b, c, d = a * scale, b * scale, c * scale, d * scale

            def eliminated(value):
                top, low = row_at(value, i), row_at(value, i + 1)
                own = d * top - b * low
                next_own = a * low - c * top
                rest = value - (one * own + two * next_own)
                return jnp.where(first, own, jnp.where(second, next_own, rest))

            for j in range(i + 2, SUB):
                spread[j] = eliminated(spread[j])
            pivot = eliminated(pivot)
        while issued < len(tasks) * (k + 1) // blocks:
            tasks[issued]()
            issued += 1
        fresh = [row_at(pivot, i) for i in range(SUB)]
        order = [(k + 1 + m) % blocks for m in range(blocks - 1)]
        for m in order:
            held = rows[m]
            terms = [held[:, base + i : base + i + 1] * fresh[i] for i in range(SUB)]
            while len(terms) > 1:
                terms = [terms[i] + terms[i + 1] for i in range(0, len(terms), 2)]
            rows[m] = jnp.where(inside, 0.0, held) - terms[0]
        rows[k] = pivot
    return jnp.concatenate(rows, axis=0)


def analysis_kernel(
    members,
    block_mask_ref,
    core_ref,
    mine_ref,
    other_ref,
    mean_ref,
    deviation_hbm,
    mean_out_ref,
    perturb_hbm,
    deviation,
    perturb,
    nothing,
    flips,
    moments,
    maps,
    transforms,
    lhs,
    in_sem,
    out_sem,
):
    bands, groups = block_mask_ref.shape
    levels = mean_ref.shape[1]
    columns = mean_ref.shape[2]
    lane = lane_of((members, LANES))
    row = row_of((members, LANES))
    diagonal = lane == row
    loads = [
        pltpu.make_async_copy(deviation_hbm.at[g], deviation.at[g], in_sem.at[g])
        for g in range(groups)
    ]
    for load in loads:
        load.start()
    nothing[...] = jnp.zeros_like(nothing)
    lower = jnp.where(
        (row_of((LANES - members, LANES)) == 0) & (lane_of((LANES - members, LANES)) == members),
        1.0,
        0.0,
    )
    for b in range(bands):
        transforms[b, pl.ds(members, LANES - members), :] = lower
    band_rows = mine_ref.shape[0] // bands
    first_core = core_ref[0] == 0

    def tile(b, q):
        pieces = []
        for core in range(2):
            low = max(q * members, core * band_rows)
            high = min((q + 1) * members, (core + 1) * band_rows)
            if low < high:
                at = pl.ds(b * band_rows + low - core * band_rows, high - low)
                mine, other = mine_ref[at, :], other_ref[at, :]
                own = first_core if core == 0 else jnp.logical_not(first_core)
                pieces.append(jnp.where(own, mine, other))
        return pieces[0] if len(pieces) == 1 else jnp.concatenate(pieces, axis=0)

    used = [0]

    def scratch():
        used[0] += 1
        return flips.at[used[0] % flips.shape[0]]

    def slot(b, s):
        return (1 << b) - 1 + s

    def unpack_first(b, q):
        def task():
            even, odd = unpack_two(tile(b, q), scratch(), members)
            moments[slot(b, 3 * q)] = even
            if 3 * q + 1 < (1 << b):
                moments[slot(b, 3 * q + 1)] = odd

        return task

    def unpack_last(b, q):
        def task():
            moments[slot(b, 3 * q + 2)] = unpack_third(tile(b, q), scratch(), members)

        return task

    def merge(stage, b, s):
        def task():
            moved = matmul(moments[slot(b, 2 * s + 1)], transforms[stage])
            square = transforms[stage, pl.ds(0, members), pl.ds(0, members)]
            moments[slot(b, s)] = moments[slot(b, 2 * s)] + matmul(square, moved)

        return task

    def update(stage):
        def task():
            if stage > 0:
                moved = matmul(maps[...], transforms[stage])
            for g in range(groups):
                at = pl.ds(g * members, members)
                if stage == 0:
                    old = jnp.where(diagonal, 1.0, 0.0)
                    new = transforms[stage, pl.ds(0, members), :]
                else:
                    old = maps[at, :]
                    new = moved[g * members : (g + 1) * members, :]
                maps[at, :] = jnp.where(block_mask_ref[stage, g] > 0, new, old)

        return task

    unpack_first(0, 0)()
    during = [[] for _ in range(bands)]
    for b in range(1, bands):
        for q in range(-(-(1 << b) // 3)):
            during[0].append(unpack_first(b, q))
            if 3 * q + 2 < (1 << b):
                during[0].append(unpack_last(b, q))
    for stage in range(bands - 1):
        for later in range(stage + 2, bands):
            for s in range(1 << (later - stage - 1)):
                during[stage + 1].append(merge(stage, later, s))
        during[stage + 1].append(update(stage))

    for b in range(bands):
        moment = moments[slot(b, 0)]
        system = jnp.where(
            lane == members, -moment, moment + jnp.where(diagonal, members - 1.0, 0.0)
        )
        solved = inverse_and_solution(system, nothing[...], members, during[b])
        transforms[b, pl.ds(0, members), :] = jnp.where(
            lane < members,
            jnp.where(diagonal, 0.5, 0.0) + (0.5 * (members - 1)) * solved,
            jnp.where(lane == members, solved, 0.0),
        )
        if b + 1 < bands:
            merge(b, b + 1, 0)()

    stores = []
    zero = jnp.zeros((2 * LANES - 3 * members, columns), jnp.bfloat16)
    update(bands - 1)()
    for g in range(groups):
        final = maps[pl.ds(g * members, members), :]
        high = final.astype(jnp.bfloat16).astype(jnp.float32)
        low = (final - high).astype(jnp.bfloat16).astype(jnp.float32)
        stack = jnp.concatenate(
            [high, low, high, jnp.zeros((2 * LANES - 3 * members, LANES), jnp.float32)], axis=0
        )
        lhs[g] = stack.T.astype(jnp.bfloat16)
    for g in range(groups):
        loads[g].wait()

        def one_level(l, carry):
            d = deviation[g, l]
            high = d.astype(jnp.bfloat16)
            low = (d - high.astype(jnp.float32)).astype(jnp.bfloat16)
            rhs = jnp.concatenate([high, high, low, zero], axis=0)
            product = jnp.dot(lhs[g], rhs, preferred_element_type=jnp.float32)
            perturb[g, l] = product[:members]
            mean_out_ref[g, pl.ds(l, 1), :] = (
                mean_ref[g, pl.ds(l, 1), :] + product[members : members + 1]
            )
            return carry

        lax.fori_loop(0, levels, one_level, 0, unroll=4)
        store = pltpu.make_async_copy(perturb.at[g], perturb_hbm.at[g], out_sem.at[g])
        store.start()
        stores.append(store)
    for store in stores:
        store.wait()


def local(
    obs_priors,
    innovation,
    obs_precision,
    tile_block,
    obs_count,
    block_mask,
    prior_state_mean,
    prior_state_deviation,
):
    members = obs_priors.shape[0]
    in_hbm = functools.partial(pltpu.with_memory_space_constraint, memory_space=pltpu.HBM)
    groups, levels, columns = prior_state_mean.shape
    bands = block_mask.shape[0]
    histories = 1 << (bands - 1)
    parts = lax.axis_size(COL)
    everyone = lax.axis_size(SAME_CORE)
    band_rows = -(-(-(-histories // 3) * members) // parts) * parts
    share = band_rows * LANES // parts
    vmem = pl.BlockSpec(memory_space=pltpu.VMEM)
    smem = pl.BlockSpec(memory_space=pltpu.SMEM)
    hbm = pl.BlockSpec(memory_space=pl.ANY)
    my_band = lax.axis_index("band").astype(jnp.int32).reshape(1)
    packed = pl.pallas_call(
        functools.partial(statistics_kernel, members),
        out_shape=jax.ShapeDtypeStruct((band_rows, LANES), jnp.float32),
        in_specs=[smem] * 4 + [vmem] * 3,
        out_specs=vmem,
        compiler_params=pltpu.CompilerParams(vmem_limit_bytes=8 << 20),
    )(
        my_band,
        in_hbm(tile_block),
        obs_count,
        in_hbm(block_mask),
        in_hbm(obs_priors),
        in_hbm(innovation.reshape(1, -1)),
        in_hbm(obs_precision.reshape(1, -1)),
    )
    received = lax.all_to_all(packed.reshape(parts, share), CORE_FIRST, 0, 0, tiled=True)
    summed = jnp.sum(received, axis=0, keepdims=True)
    copies = jnp.broadcast_to(summed, (everyone, share))
    mine = lax.all_to_all(copies, SAME_CORE, 0, 0, tiled=True).reshape(-1, LANES)
    other = lax.ppermute(mine, CORE, [(0, 1), (1, 0)])
    my_core = lax.axis_index(CORE).astype(jnp.int32).reshape(1)
    return pl.pallas_call(
        functools.partial(analysis_kernel, members),
        out_shape=(
            jax.ShapeDtypeStruct(prior_state_mean.shape, jnp.float32),
            jax.ShapeDtypeStruct(prior_state_deviation.shape, jnp.float32),
        ),
        in_specs=[smem, smem, vmem, vmem, vmem, hbm],
        out_specs=(vmem, hbm),
        scratch_shapes=[
            pltpu.VMEM(prior_state_deviation.shape, jnp.float32),
            pltpu.VMEM(prior_state_deviation.shape, jnp.float32),
            pltpu.VMEM((SUB, LANES), jnp.float32),
            pltpu.VMEM((4, LANES, LANES), jnp.float32),
            pltpu.VMEM(((1 << bands) - 1, members, LANES), jnp.float32),
            pltpu.VMEM((groups * members, LANES), jnp.float32),
            pltpu.VMEM((bands, LANES, LANES), jnp.float32),
            pltpu.VMEM((groups, LANES, 2 * LANES), jnp.bfloat16),
            pltpu.SemaphoreType.DMA((groups,)),
            pltpu.SemaphoreType.DMA((groups,)),
        ],
        compiler_params=pltpu.CompilerParams(vmem_limit_bytes=50 << 20),
    )(in_hbm(block_mask), my_core, mine, other, in_hbm(prior_state_mean), in_hbm(prior_state_deviation))


def solution(mesh):
    cols = mesh.shape["col"]
    shape = (mesh.shape["band"], cols // 8, 4, 2) if cols % 8 == 0 else (mesh.shape["band"], 1, 1, cols)
    torus = Mesh(mesh.devices.reshape(shape), BAND_COL)
    placed = (
        P(None, BAND_COL),
        P(BAND_COL),
        P(BAND_COL),
        P(BAND_COL),
        P(BAND_COL),
        P(None, COL),
        P(COL, None, "band"),
        P(COL, None, None, "band"),
    )
    return jax.shard_map(
        local,
        mesh=torus,
        in_specs=placed,
        out_specs=(P(COL, None, "band"), P(COL, None, None, "band")),
        check_vma=False,
    )
```
